32 devices in a mesh: scen: 8 (over y, x, core), col: 4 (over z).
Axes of the slice: x: 2, y: 2, z: 4, core: 2. Of those that a mesh axis runs over, the one named last changes fastest.
Arguments:
- tech: bfloat16 [32, 2048, 4096], P('scen', None, 'col'), may hold values from -0.046875 to 0.046875
- recourse: bfloat16 [32, 2048, 1024], P('scen', None, 'col'), may hold values from -0.125 to 0.125
- rhs: float32 [32, 32, 2048], P(None, 'scen'), may hold values from -6 to 6
- cost_first: float32 [4096], P('col'), may hold values from -6 to 6
- cost_second: float32 [32, 1024], P('scen', 'col'), may hold values from -6 to 6
- cone_id: int32 [32, 2048], P('scen'), may hold values from 0 to 127, never falling along the last dimension, each value on 1 to 64 neighbouring positions
Outputs:
- first_section: float32 [32, 4096], P(None, 'col')
- second_section: float32 [32, 32, 1024], P(None, 'scen', 'col')
- slack: float32 [32, 32, 2048], P(None, 'scen', 'col')
- dual: float32 [32, 32, 2048], P(None, 'scen', 'col')
The draws below stay inside these ranges and needn't reach their ends.
Inputs may be any that keep to these rules, and one draw needn't show every extreme that they name: Along the rows of a scenario cone_id never falls; a cone holds 1 to 64 rows.
All inputs are finite; a program needn't handle non-finite values.
Results may differ from the reference program's by a relative error of at most 0.014.
Values may be sent and summed in bfloat16 or wider, within the bound.
No kernel may reach another device: no remote copies, remote signals or barrier semaphores. Data moves between devices by JAX's collectives and lax.ppermute only.
A program may use at most 128 MiB of HBM per device.

```python
import math
import jax
import jax.numpy as jnp
import numpy as np
from jax import lax

M = 2048
NX = 4096
NY = 1024
NCONE = 128
CONE_MOST = 64
BATCH = 32
ITERS = 3
CG_STEPS = 3
SCENS = 32


def steps_of(key, shape, cuts, least, top_value):
    def one(dim, parts):
        draws = jax.random.uniform(jax.random.fold_in(jax.random.fold_in(key, 6), dim), (parts,), jnp.float32, least / len(cuts), top_value / len(cuts))
        return jnp.repeat(jnp.exp(draws), shape[dim] // parts).reshape((-1,) + (1,) * (len(shape) - dim - 1))

    gain = one(*cuts[0])
    for cut in cuts[1:]:
        gain = gain * one(*cut)
    return gain


def split_up(count, total, reach, slope):
    loads = [(1 << 20) // math.isqrt(grade ** slope) + 1 for grade in range(2, count + 1)]
    spare, holding = total - reach - (count - 1), [1] * (count - 1)
    while spare > 0:
        candidates = [i for i in range(count - 1) if holding[i] < reach]
        whole, left = sum([loads[i] for i in candidates]), spare
        for i in candidates:
            more = min(reach - holding[i], max(1, left * loads[i] // whole), spare)
            holding[i] = holding[i] + more
            spare = spare - more
    return np.array([reach] + holding)


def uneven_parts(rng, number_of, total, limit, lean):
    if number_of == 2:
        one = jax.random.randint(rng, (), max(1, total - limit), min(limit, total - 1) + 1)
        return jnp.stack([one, total - one])
    tallies = jnp.asarray(split_up(number_of, total, limit, lean), jnp.int32)
    couples = (number_of - 1) // 2
    source_of, receiver = tallies[1:1 + 2 * couples:2], tallies[2:2 + 2 * couples:2]
    room = jnp.minimum(source_of - 1, limit - receiver)
    moved = jax.random.randint(jax.random.fold_in(rng, 1), (couples,), 0, 1 << 20) % (room + 1)
    tallies = tallies.at[1:1 + 2 * couples:2].set(source_of - moved).at[2:2 + 2 * couples:2].set(receiver + moved)
    return tallies[jax.random.permutation(jax.random.fold_in(rng, 2), number_of)]


def bell_draw(key, shape, spread, reach, split=(), dtype=jnp.bfloat16):
    loudness = steps_of(key, shape, split, -0.22, 0.18) if split else 1.0
    entries = jax.random.normal(key, shape, jnp.float32) * spread * loudness
    return jnp.minimum(jnp.maximum(entries, -reach), reach).astype(dtype)


def setup_inputs(seed: int = 0) -> dict:
    key_of = jax.random.split(jax.random.key(seed), 7)
    tech = bell_draw(key_of[0], (SCENS, M, NX), (SCENS * M // 4) ** -0.5, 0.046875, ((0, 8), (2, 4)))
    recourse = bell_draw(key_of[1], (SCENS, M, NY), M ** -0.5, 0.125, ((0, 8), (2, 4)))
    rhs = bell_draw(key_of[2], (BATCH, SCENS, M), 1.0, 6.0, ((1, 8),), jnp.float32)
    cost_first = bell_draw(key_of[3], (NX,), 1.0, 6.0, ((0, 4),), jnp.float32)
    cost_second = bell_draw(key_of[4], (SCENS, NY), 1.0, 6.0, ((0, 8), (1, 4)), jnp.float32)
    cone_id = jax.vmap(lambda own: jnp.searchsorted(jnp.cumsum(uneven_parts(own, NCONE, M, CONE_MOST, 2)), jnp.arange(M), side="right"))(jax.random.split(key_of[5], SCENS)).reshape((SCENS, M)).astype(jnp.int32)
    return dict(tech=tech, recourse=recourse, rhs=rhs, cost_first=cost_first, cost_second=cost_second, cone_id=cone_id)


HIGH = lax.Precision.HIGHEST

def cone_factors(lead, tail):
    norm_tail = jnp.sqrt(tail)
    inside = norm_tail <= lead
    polar = norm_tail <= -lead
    safe = jnp.where(norm_tail > 0.0, norm_tail, 1.0)
    middle = 0.5 * (lead + norm_tail)
    head = jnp.where(inside, lead, jnp.where(polar, 0.0, middle))
    scale = jnp.where(inside, 1.0, jnp.where(polar, 0.0, middle / safe))
    return (head, scale)

def reference(tech, recourse, rhs, cost_first, cost_second, cone_id):
    f32 = jnp.float32
    bf16 = jnp.bfloat16
    batch = rhs.shape[0]
    scen_count = tech.shape[0]
    rows = tech.shape[1]
    rhs_s = jnp.transpose(rhs, (1, 0, 2))
    starts = jnp.concatenate([jnp.ones((scen_count, 1), f32), (cone_id[:, 1:] != cone_id[:, :-1]).astype(f32)], axis=1)
    labels = lax.broadcasted_iota(jnp.int32, (1, 1, NCONE), 2)
    onehot = (cone_id[:, :, None] == labels).astype(f32)
    start_rows = starts[:, None, :]

    def project(values):
        lead = jnp.einsum('sbm,smc->sbc', values * start_rows, onehot, precision=HIGH)
        tail = jnp.einsum('sbm,smc->sbc', values * values * (1.0 - start_rows), onehot, precision=HIGH)
        head, scale = cone_factors(lead, tail)
        head_rows = jnp.einsum('sbc,smc->sbm', head, onehot, precision=HIGH)
        scale_rows = jnp.einsum('sbc,smc->sbm', scale, onehot, precision=HIGH)
        return start_rows * head_rows + (1.0 - start_rows) * values * scale_rows

    def forward(dir_first_bf, dir_second_bf):

        def single(args):
            tech_s, rec_s, dir_s = args
            return jnp.dot(dir_first_bf, tech_s.T, preferred_element_type=f32) + jnp.dot(dir_s, rec_s.T, preferred_element_type=f32)
        return lax.map(single, (tech, recourse, dir_second_bf))

    def adjoint(rows_bf):

        def single(carry, args):
            tech_s, rec_s, rows_s = args
            return (carry + jnp.dot(rows_s, tech_s, preferred_element_type=f32), jnp.dot(rows_s, rec_s, preferred_element_type=f32))
        return lax.scan(single, jnp.zeros((batch, tech.shape[2]), f32), (tech, recourse, rows_bf))

    def squares(first_vec, second_vec):
        return lax.optimization_barrier(jnp.sum(first_vec * first_vec, axis=1)) + lax.optimization_barrier(jnp.sum(second_vec * second_vec, axis=(0, 2)))
    first_sol = jnp.zeros((batch, tech.shape[2]), f32)
    second_sol = jnp.zeros((scen_count, batch, recourse.shape[2]), f32)
    slack = jnp.zeros((scen_count, batch, rows), f32)
    dual = jnp.zeros((scen_count, batch, rows), f32)
    image = jnp.zeros((scen_count, batch, rows), f32)
    for outer in range(ITERS):
        resid_rows = (rhs_s - slack - dual - image).astype(bf16)
        back_first, back_second = adjoint(resid_rows)
        res_first = back_first - cost_first[None, :]
        res_second = back_second - cost_second[:, None, :]
        res_norm = squares(res_first, res_second)
        dir_first, dir_second = (res_first, res_second)
        for step in range(CG_STEPS):
            image_step = forward(dir_first.astype(bf16), dir_second.astype(bf16))
            curv = squares(dir_first, dir_second) + lax.optimization_barrier(jnp.sum(image_step * image_step, axis=(0, 2)))
            alpha = res_norm / curv
            first_sol = first_sol + alpha[:, None] * dir_first
            second_sol = second_sol + alpha[None, :, None] * dir_second
            image = image + alpha[None, :, None] * image_step
            if step + 1 < CG_STEPS:
                back_first, back_second = adjoint(image_step.astype(bf16))
                res_first = res_first - alpha[:, None] * (dir_first + back_first)
                res_second = res_second - alpha[None, :, None] * (dir_second + back_second)
                new_norm = squares(res_first, res_second)
                ratio = new_norm / res_norm
                dir_first = res_first + ratio[:, None] * dir_first
                dir_second = res_second + ratio[None, :, None] * dir_second
                res_norm = new_norm
        slack = project(rhs_s - image - dual)
        dual = dual + image + slack - rhs_s
    return (first_sol, jnp.transpose(second_sol, (1, 0, 2)), jnp.transpose(slack, (1, 0, 2)), jnp.transpose(dual, (1, 0, 2)))
```

```python
import functools

import jax
import jax.numpy as jnp
from jax import lax
from jax.experimental import pallas as pl
from jax.experimental.pallas import tpu as pltpu
from jax.sharding import PartitionSpec as P

NCONE = 128
ITERS = 3
CG_STEPS = 3
GROUPS = 2
LANES = 128
EXTRA = 8


F32 = jnp.float32
BF16 = jnp.bfloat16
VMEM = pl.BlockSpec(memory_space=pltpu.VMEM)
SMEM = pl.BlockSpec(memory_space=pltpu.SMEM)
BIG = 26 << 20
SMALL = 12 << 20


def swap(value, axis, size, k):
    return lax.ppermute(value, axis, [(j, j ^ k) for j in range(size)])


def tree_sum(parts):
    while len(parts) > 1:
        parts = [parts[j] + parts[j + 1] for j in range(0, len(parts), 2)]
    return parts[0]


def call(kernel, name, out_shape, args, limit=SMALL, aliases=None, smem=0, cost=(10**6, 10**6)):
    return pl.pallas_call(
        kernel,
        name=name,
        in_specs=[SMEM] * smem + [VMEM] * (len(args) - smem),
        out_specs=[VMEM] * len(out_shape),
        out_shape=out_shape,
        input_output_aliases=aliases or {},
        compiler_params=pltpu.CompilerParams(vmem_limit_bytes=limit),
        cost_estimate=pl.CostEstimate(flops=cost[0], bytes_accessed=cost[1], transcendentals=0),
    )(*args)


def struct(shape, dtype=F32):
    return jax.ShapeDtypeStruct(tuple(shape), dtype)


def chunk(ids, k, w):
    return pl.ds(pl.multiple_of(ids[k] * w, w), w)


def split3(v):
    hi = v.astype(BF16)
    rest = v - hi.astype(F32)
    mid = rest.astype(BF16)
    low = (rest - mid.astype(F32)).astype(BF16)
    return hi, mid, low


def at_lane(shape, j, column):
    return jnp.where(lax.broadcasted_iota(jnp.int32, shape, 1) == j, column, 0.0)


def forward_kernel(s0, sg, has_block, ids, *refs):
    if has_block:
        block_ref, refs = refs[0], refs[1:]
    x_ref, y_ref, t_ref, w_ref, own_ref, *out_refs = refs
    w = own_ref.shape[2]
    batch = x_ref.shape[0]
    dn = (((1,), (1,)), ((), ()))

    def one(s, _):
        for k in list(range(1, len(out_refs) + 1)) + [0]:
            r = chunk(ids, k, w)
            z = lax.dot_general(t_ref[s0 + s, r], x_ref[...], dn, preferred_element_type=F32)
            z = z + lax.dot_general(w_ref[s0 + s, r], y_ref[s0 + s], dn, preferred_element_type=F32)
            if k == 0:
                own_ref[s] = z.T
            else:
                out_refs[k - 1][pl.ds(pl.multiple_of(s * batch, batch), batch)] = z.T.astype(BF16)
        return 0

    lax.fori_loop(0, sg, one, 0)
    if has_block:
        for ref in out_refs:
            ref[pl.ds(sg * batch, EXTRA)] = block_ref[...]


def forward(ids, block, x_bf, y_bf, tech, recourse, s0, sg, n):
    batch, first_cols = x_bf.shape
    second_cols = y_bf.shape[2]
    w = tech.shape[1] // n
    sent = (sg * batch + (0 if block is None else EXTRA), w)
    args = [ids] + ([] if block is None else [block]) + [x_bf, y_bf, tech, recourse]
    work = sg * n * w * (first_cols + second_cols)
    return call(
        functools.partial(forward_kernel, s0, sg, block is not None),
        "forward",
        [struct((sg, batch, w))] + [struct(sent, BF16)] * (n - 1),
        args, BIG, smem=1, cost=(2 * batch * work * 8, 2 * work),
    )


def gather_kernel(n, has_block, *refs):
    if has_block:
        block_ref, refs = refs[0], refs[1:]
    own_ref, *others = refs[:n]
    total_ref = refs[n]
    sg, batch, w = own_ref.shape
    for s in range(sg):
        rows = pl.ds(s * batch, batch)
        total_ref[s] = (own_ref[s] + sum(o[rows].astype(F32) for o in others)).astype(BF16)
    if has_block:
        scal_ref = refs[n + 1]
        rows = pl.ds(sg * batch, EXTRA)
        parts = []
        for p in [block_ref[:, :LANES]] + [o[rows, :LANES] for o in others]:
            p = p.astype(F32)
            parts.append((p + pltpu.roll(p, EXTRA - 2, 0)) + pltpu.roll(p, EXTRA - 4, 0))
        both = tree_sum(parts)
        square = jnp.concatenate([both, jnp.zeros((LANES - EXTRA, LANES), F32)], axis=0).T
        lane = lax.broadcasted_iota(jnp.int32, (batch, LANES), 1)
        scal_ref[...] = jnp.where(lane < 2, square[:batch], 0.0)


def gather(block, own, received):
    n = len(received) + 1
    args = ([] if block is None else [block]) + [own, *received]
    out = [struct(own.shape, BF16)]
    if block is not None:
        out.append(struct((own.shape[1], LANES)))
    return call(functools.partial(gather_kernel, n, block is not None), "gather", out, args)


def adjoint_kernel(n, s0, has_q, ids, *refs):
    z_refs, refs = refs[:n], refs[n:]
    if has_q:
        q_ref, refs = refs[0], refs[1:]
    acc_ref, t_ref, w_ref, out_ref, ty_ref = refs
    sg, batch, w = z_refs[0].shape
    cols = t_ref.shape[2]
    if acc_ref.shape[1] > LANES:
        out_ref[:, :cols] = acc_ref[:, :cols]
    else:
        out_ref[:, :cols] = jnp.zeros((batch, cols), F32)

    def one(s, carry):
        zz, zq = carry
        ty = jnp.zeros((batch, w_ref.shape[2]), F32)
        acc = out_ref[:, :cols]
        for k in range(n):
            r = chunk(ids, k, w)
            z = z_refs[k][s]
            ty = ty + jnp.dot(z, w_ref[s0 + s, r], preferred_element_type=F32)
            acc = acc + jnp.dot(z, t_ref[s0 + s, r], preferred_element_type=F32)
            zf = z.astype(F32)
            zz = zz + zf * zf
            if has_q:
                zq = zq + zf * q_ref[k, s0 + s]
        ty_ref[s] = ty
        out_ref[:, :cols] = acc
        return zz, zq

    zero = jnp.zeros((batch, w), F32)
    zz, zq = lax.fori_loop(0, sg, one, (zero, zero))
    scal = acc_ref[:, acc_ref.shape[1] - LANES:]
    scal = scal + at_lane(scal.shape, 2, jnp.sum(zz, axis=1, keepdims=True))
    if has_q:
        scal = scal + at_lane(scal.shape, 3, jnp.sum(zq, axis=1, keepdims=True))
    out_ref[:, cols:] = scal


def adjoint(ids, pieces, q, acc, tech, recourse, s0):
    n = len(pieces)
    sg, batch, w = pieces[0].shape
    first_cols = tech.shape[2]
    second_cols = recourse.shape[2]
    args = [ids, *pieces] + ([] if q is None else [q]) + [acc, tech, recourse]
    work = sg * n * w * (first_cols + second_cols)
    return call(
        functools.partial(adjoint_kernel, n, s0, q is not None),
        "adjoint",
        [struct((batch, first_cols + LANES)), struct((sg, batch, second_cols))],
        args, BIG, smem=1, cost=(2 * batch * work * 8, 2 * work),
    )


def pack_kernel(a_ref, b_ref, out_ref):
    cols = a_ref.shape[1] - LANES
    out_ref[:, :cols] = (a_ref[:, :cols] + b_ref[:, :cols]).astype(BF16)
    hi, mid, low = (p.astype(F32) for p in split3(a_ref[:, cols:] + b_ref[:, cols:]))
    out_ref[:, cols:] = (hi + pltpu.roll(mid, 4, 1) + pltpu.roll(low, 8, 1)).astype(BF16)


def sum_far(part_refs):
    cols = part_refs[0].shape[1] - LANES
    vector = tree_sum([p[:, :cols].astype(F32) for p in part_refs])
    scal = []
    for p in part_refs:
        t = p[:, cols:].astype(F32)
        scal.append((t + pltpu.roll(t, LANES - 4, 1)) + pltpu.roll(t, LANES - 8, 1))
    return vector, tree_sum(scal)


def write_block(block_ref, norm, cross):
    batch = norm.shape[0]
    shape = (LANES, LANES)
    pieces = [p.astype(F32) for p in split3(norm)] + [p.astype(F32) for p in split3(cross)]
    square = jnp.zeros((batch, LANES), F32)
    for j, p in enumerate((pieces[0], pieces[3], pieces[1], pieces[4], pieces[2], pieces[5])):
        square = square + at_lane((batch, LANES), j, p)
    square = jnp.concatenate([square, jnp.zeros((LANES - batch, LANES), F32)], axis=0).T
    block_ref[...] = jnp.zeros_like(block_ref)
    block_ref[:, :LANES] = square[:EXTRA].astype(BF16)


def rowsum(v):
    return jnp.sum(v, axis=1, keepdims=True)


def begin_kernel(n_far, share, *refs):
    parts, refs = refs[:n_far], refs[n_far:]
    ty_ref, cx_ref, cy_ref, rx_ref, ry_ref, xb_ref, yb_ref, block_ref = refs
    vector, _ = sum_far(parts)
    res = vector - cx_ref[...]
    rx_ref[...] = res
    xb_ref[...] = res.astype(BF16)
    norm = rowsum(res * res) * share
    for s in range(ty_ref.shape[0]):
        res = ty_ref[s] - cy_ref[s]
        ry_ref[s] = res
        yb_ref[s] = res.astype(BF16)
        norm = norm + rowsum(res * res)
    write_block(block_ref, norm, norm)


def steps_of(step, scal, st):
    norm, cross, zz, zq = (scal[:, j:j + 1] for j in range(4))
    if step:
        old_norm, dd, qq = (st[:, j:j + 1] for j in range(3))
        beta = norm / old_norm
        dd = norm + 2.0 * beta * cross + beta * beta * dd
        qq = zz + 2.0 * beta * zq + beta * beta * qq
    else:
        beta = jnp.zeros_like(norm)
        dd, qq = norm, zz
    alpha = norm / (dd + qq)
    shape = scal.shape
    st = at_lane(shape, 0, norm) + at_lane(shape, 1, dd) + at_lane(shape, 2, qq)
    ab = at_lane(shape, 0, alpha) + at_lane(shape, 1, beta)
    return alpha, beta, st, ab


def update_kernel(n_far, step, share, *refs):
    parts, refs = refs[:n_far], refs[n_far:]
    if step:
        st_ref, dx_ref, dy_ref, mx_ref, my_ref = refs[:5]
        refs = refs[5:]
    ty_ref, rx_ref, ry_ref, solx_ref, soly_ref = refs[:5]
    (rxo, ryo, dxo, dyo, mxo, myo, solxo, solyo, sto, abo, xb_ref, yb_ref, block_ref) = refs[5:]
    vector, scal = sum_far(parts)
    alpha, beta, st, ab = steps_of(step, scal, st_ref[...] if step else None)
    sto[...] = st
    abo[...] = ab

    def one(res, t, d, m):
        if step:
            m = (res + t) + beta * m
            d = res + beta * d
        else:
            m = res + t
            d = res
        return res - alpha * m, d, m

    old = (dx_ref[...], mx_ref[...]) if step else (None, None)
    res, d, m = one(rx_ref[...], vector, *old)
    rxo[...] = res
    dxo[...] = d
    mxo[...] = m
    solxo[...] = solx_ref[...] + alpha * d
    xb_ref[...] = res.astype(BF16)
    norm = rowsum(res * res) * share
    cross = rowsum(res * d) * share
    for s in range(ty_ref.shape[0]):
        old = (dy_ref[s], my_ref[s]) if step else (None, None)
        res, d, m = one(ry_ref[s], ty_ref[s], *old)
        ryo[s] = res
        dyo[s] = d
        myo[s] = m
        solyo[s] = soly_ref[s] + alpha * d
        yb_ref[s] = res.astype(BF16)
        norm = norm + rowsum(res * res)
        cross = cross + rowsum(res * d)
    write_block(block_ref, norm, cross)


def row_kernel(n, groups, step, *refs):
    z_refs, refs = refs[:n * groups], refs[n * groups:]
    if step:
        q_ref, refs = refs[0], refs[1:]
    image_ref, ab_ref, qo, imageo = refs
    sg = z_refs[0].shape[0]
    ab = ab_ref[...]
    alpha, beta = ab[:, 0:1], ab[:, 1:2]

    def one(s, _):
        for g in range(groups):
            for k in range(n):
                q = z_refs[g * n + k][s].astype(F32)
                if step:
                    q = q + beta * q_ref[k, g * sg + s]
                qo[k, g * sg + s] = q
                imageo[k, g * sg + s] = image_ref[k, g * sg + s] + alpha * q
        return 0

    lax.fori_loop(0, sg, one, 0)


def rowscal_kernel(n, groups, *refs):
    z_refs, refs = refs[:n * groups], refs[n * groups:]
    q_ref, scal_ref, out_ref = refs
    sg, batch, w = z_refs[0].shape

    def one(s, carry):
        zz, zq = carry
        for g in range(groups):
            for k in range(n):
                z = z_refs[g * n + k][s].astype(F32)
                zz = zz + z * z
                zq = zq + z * q_ref[k, g * sg + s]
        return zz, zq

    zero = jnp.zeros((batch, w), F32)
    zz, zq = lax.fori_loop(0, sg, one, (zero, zero))
    shape = out_ref.shape
    out_ref[...] = scal_ref[...] + at_lane(shape, 2, rowsum(zz)) + at_lane(shape, 3, rowsum(zq))


def finish_kernel(n_far, *refs):
    parts, refs = refs[:n_far], refs[n_far:]
    st_ref, dx_ref, dy_ref, rx_ref, ry_ref, solx_ref, soly_ref, solxo, solyo, abo = refs
    alpha, beta, _, ab = steps_of(1, tree_sum([p[...] for p in parts]), st_ref[...])
    abo[...] = ab
    solxo[...] = solx_ref[...] + alpha * (rx_ref[...] + beta * dx_ref[...])
    for s in range(ry_ref.shape[0]):
        solyo[s] = soly_ref[s] + alpha * (ry_ref[s] + beta * dy_ref[s])


def cone_factors(lead, tail):
    norm_tail = jnp.sqrt(tail)
    inside = norm_tail <= lead
    polar = norm_tail <= -lead
    safe = jnp.where(norm_tail > 0.0, norm_tail, 1.0)
    middle = 0.5 * (lead + norm_tail)
    head = jnp.where(inside, lead, jnp.where(polar, 0.0, middle))
    scale = jnp.where(inside, 1.0, jnp.where(polar, 0.0, middle / safe))
    return head, scale


def project_kernel(n, groups, *refs):
    z_refs, refs = refs[:n * groups], refs[n * groups:]
    q_ref, image_ref, ab_ref, rhs_ref, dual_ref, cone_ref, start_ref = refs[:7]
    imageo_ref, slack_ref, dualo_ref, *d_refs = refs[7:]
    _, scen, b, w = rhs_ref.shape
    sg = scen // groups
    labels = lax.broadcasted_iota(jnp.int32, (NCONE, w), 0)
    ab = ab_ref[...]
    alpha, beta = ab[:, 0:1], ab[:, 1:2]
    for g in range(groups):
        def one(j, _, g=g):
            s = g * sg + j
            values = []
            images = []
            sums = jnp.zeros((6 * b, NCONE), F32)
            for k in range(n):
                image = image_ref[k, s] + alpha * (z_refs[g * n + k][j].astype(F32) + beta * q_ref[k, s])
                imageo_ref[k, s] = image
                v = rhs_ref[k, s] - image - dual_ref[k, s]
                st = start_ref[k, s]
                onehot = (cone_ref[k, s] == labels).astype(F32).astype(BF16)
                stack = jnp.concatenate(split3(v * st) + split3(v * v * (1.0 - st)), axis=0)
                sums = sums + lax.dot_general(
                    stack, onehot, (((1,), (1,)), ((), ())), preferred_element_type=F32
                )
                values.append(v)
                images.append(image)
            lead = (sums[2 * b:3 * b] + sums[b:2 * b]) + sums[:b]
            tail = (sums[5 * b:6 * b] + sums[4 * b:5 * b]) + sums[3 * b:4 * b]
            head, scale = cone_factors(lead, tail)
            back = jnp.concatenate(split3(head) + split3(scale), axis=0)
            for k in range(n):
                onehot = (cone_ref[k, s] == labels).astype(F32).astype(BF16)
                rows = jnp.dot(back, onehot, preferred_element_type=F32)
                head_rows = (rows[2 * b:3 * b] + rows[b:2 * b]) + rows[:b]
                scale_rows = (rows[5 * b:6 * b] + rows[4 * b:5 * b]) + rows[3 * b:4 * b]
                st = start_ref[k, s]
                slack = st * head_rows + (1.0 - st) * values[k] * scale_rows
                base = images[k] - rhs_ref[k, s]
                dual = dual_ref[k, s] + base + slack
                if k == 0:
                    slack_ref[s] = slack
                dualo_ref[k, s] = dual
                d_refs[g * n + k][j] = (-base - slack - dual).astype(BF16)
            return 0

        lax.fori_loop(0, sg, one, 0)


def body(tech, recourse, rhs, cost_first, cost_second, cone_id):
    n_scen = lax.axis_size("scen")
    n = lax.axis_size("col")
    here = lax.axis_index("col")
    scen, rows, first_cols = tech.shape
    second_cols = recourse.shape[2]
    batch = rhs.shape[0]
    w = rows // n
    sg = scen // GROUPS
    share = 1.0 / n_scen
    ids = (here ^ jnp.arange(n, dtype=jnp.int32)).astype(jnp.int32)

    def ordered(value):
        parts = [lax.dynamic_slice_in_dim(value, (here ^ k) * w, w, value.ndim - 1) for k in range(n)]
        return jnp.stack(parts)

    rhs_k = ordered(jnp.transpose(rhs, (1, 0, 2)))
    start = jnp.concatenate(
        [jnp.ones((scen, 1), F32), (cone_id[:, 1:] != cone_id[:, :-1]).astype(F32)], axis=1
    )
    start_k = ordered(start)[:, :, None, :]
    cone_k = ordered(cone_id)[:, :, None, :]
    cost_x = cost_first[None, :]
    cost_y = cost_second[:, None, :]

    far = list(range(2, n_scen, 2))
    n_far = len(far) + 1
    first_shape = struct((batch, first_cols))
    second_shape = struct((scen, batch, second_cols))
    scal_shape = struct((batch, LANES))
    block_shape = struct((EXTRA, w), BF16)
    cast_shapes = [struct(first_shape.shape, BF16), struct(second_shape.shape, BF16), block_shape]

    def far_parts(own):
        return [own] + [swap(own, "scen", n_scen, k) for k in far]

    def reduce_first(payload):
        other = swap(payload, "scen", n_scen, 1)
        (own,) = call(pack_kernel, "pack", [struct(payload.shape, BF16)], [payload, other])
        return far_parts(own)

    def apply_forward(x_bf, y_bf, block):
        groups = []
        scal = None
        for g in range(GROUPS):
            own, *others = forward(
                ids, block if g == 0 else None, x_bf, y_bf, tech, recourse, g * sg, sg, n
            )
            received = [swap(part, "col", n, k + 1) for k, part in enumerate(others)]
            total = gather(block if g == 0 else None, own, received)
            if g == 0:
                scal = total[1]
            total = total[0]
            groups.append([total] + [swap(total, "col", n, k) for k in range(1, n)])
        return groups, scal

    def apply_adjoint(groups, q, acc):
        seconds = []
        for g, pieces in enumerate(groups):
            acc, second = adjoint(ids, pieces, q, acc, tech, recourse, g * sg)
            seconds.append(second)
        return acc, seconds[0] if GROUPS == 1 else jnp.concatenate(seconds, axis=0)

    flat = lambda groups: [piece for pieces in groups for piece in pieces]
    sol_first = jnp.zeros(first_shape.shape, F32)
    sol_second = jnp.zeros(second_shape.shape, F32)
    dual = jnp.zeros(rhs_k.shape, F32)
    image = jnp.zeros(rhs_k.shape, F32)
    no_scal = jnp.zeros((batch, LANES), F32)
    d = rhs_k.astype(BF16)
    groups = [[d[k, g * sg:(g + 1) * sg] for k in range(n)] for g in range(GROUPS)]
    for outer in range(ITERS):
        payload, ty = apply_adjoint(groups, None, no_scal)
        parts = reduce_first(payload)
        rx, ry, x_bf, y_bf, block = call(
            functools.partial(begin_kernel, n_far, share), "begin",
            [first_shape, second_shape] + cast_shapes, parts + [ty, cost_x, cost_y],
        )
        q = None
        state = []
        for step in range(CG_STEPS):
            groups, scal = apply_forward(x_bf, y_bf, block)
            if step + 1 < CG_STEPS:
                payload, ty = apply_adjoint(groups, q, scal)
                parts = reduce_first(payload)
                (rx, ry, dx, dy, mx, my, sol_first, sol_second, st, ab, x_bf, y_bf, block) = call(
                    functools.partial(update_kernel, n_far, step, share), "update",
                    [first_shape, second_shape] * 4 + [scal_shape] * 2 + cast_shapes,
                    parts + state + [ty, rx, ry, sol_first, sol_second],
                )
                state = [st, dx, dy, mx, my]
                q, image = call(
                    functools.partial(row_kernel, n, GROUPS, step), "rows",
                    [struct(image.shape)] * 2,
                    flat(groups) + ([] if q is None else [q]) + [image, ab],
                )
            else:
                (scal,) = call(
                    functools.partial(rowscal_kernel, n, GROUPS), "rowscal", [scal_shape],
                    flat(groups) + [q, scal],
                )
                parts = far_parts(scal + swap(scal, "scen", n_scen, 1))
                sol_first, sol_second, ab = call(
                    functools.partial(finish_kernel, n_far), "finish",
                    [first_shape, second_shape, scal_shape],
                    parts + [st, dx, dy, rx, ry, sol_first, sol_second],
                )
        image, slack, dual, *ds = call(
            functools.partial(project_kernel, n, GROUPS), "project",
            [struct(image.shape), struct(image.shape[1:]), struct(image.shape)]
            + [struct((sg, batch, w), BF16)] * (n * GROUPS),
            flat(groups) + [q, image, ab, rhs_k, dual, cone_k, start_k], 20 << 20,
        )
        groups = [ds[g * n:(g + 1) * n] for g in range(GROUPS)]
    swap_lead = lambda value: jnp.transpose(value, (1, 0, 2))
    return sol_first, swap_lead(sol_second), swap_lead(slack), swap_lead(dual[0])


def solution(mesh):
    placed = (
        P("scen", None, "col"),
        P("scen", None, "col"),
        P(None, "scen", None),
        P("col"),
        P("scen", "col"),
        P("scen", None),
    )
    return jax.shard_map(
        body,
        mesh=mesh,
        in_specs=placed,
        out_specs=(
            P(None, "col"),
            P(None, "scen", "col"),
            P(None, "scen", "col"),
            P(None, "scen", "col"),
        ),
        check_vma=False,
    )
```

```python
import functools

import jax
import jax.numpy as jnp
from jax import lax
from jax.experimental import pallas as pl
from jax.experimental.pallas import tpu as pltpu
from jax.sharding import PartitionSpec as P


NCONE = 128
ITERS = 3
CG_STEPS = 3
SIZES = (1, 2, 1)
GROUPS = len(SIZES)
FIRST = tuple(sum(SIZES[:g]) for g in range(GROUPS))
ORDER = (
    ("forward", 0),
    ("forward", 1),
    ("pair", 0),
    ("forward", 2),
    ("pair", 1),
    ("total", 0),
    ("pair", 2),
    ("total", 1),
    ("adjoint", 0),
    ("total", 2),
    ("adjoint", 1),
    ("adjoint", 2),
)
LANES = 128
EXTRA = 8


F32 = jnp.float32
BF16 = jnp.bfloat16
VMEM = pl.BlockSpec(memory_space=pltpu.VMEM)
SMEM = pl.BlockSpec(memory_space=pltpu.SMEM)
ANY = pl.BlockSpec(memory_space=pl.ANY)
HBM = pl.BlockSpec(memory_space=pltpu.HBM)
BIG = 6 << 20
SMALL = 4 << 20


def swap(value, axis, size, k):
    return lax.ppermute(value, axis, [(j, j ^ k) for j in range(size)])


def tree_sum(parts):
    while len(parts) > 1:
        parts = [parts[j] + parts[j + 1] for j in range(0, len(parts), 2)]
    return parts[0]


def call(kernel, out_shape, args, limit=SMALL, smem=0, cost=(10**6, 10**6), after=()):
    count = len(args)

    def ordered_kernel(*refs):
        kernel(*refs[:count], *refs[count + len(after):])

    return pl.pallas_call(
        ordered_kernel if after else kernel,
        in_specs=[SMEM] * smem + [VMEM] * (count - smem) + [ANY] * len(after),
        out_specs=[VMEM] * len(out_shape),
        out_shape=out_shape,
        compiler_params=pltpu.CompilerParams(vmem_limit_bytes=limit),
        cost_estimate=pl.CostEstimate(flops=cost[0], bytes_accessed=cost[1], transcendentals=0),
    )(*args, *after)


def struct(shape, dtype=F32):
    return jax.ShapeDtypeStruct(tuple(shape), dtype)


def chunk(ids, k, w):
    return pl.ds(pl.multiple_of(ids[k] * w, w), w)


def split3(v):
    hi = v.astype(BF16)
    rest = v - hi.astype(F32)
    mid = rest.astype(BF16)
    low = (rest - mid.astype(F32)).astype(BF16)
    return hi, mid, low


def at_lane(shape, j, column):
    return jnp.where(lax.broadcasted_iota(jnp.int32, shape, 1) == j, column, 0.0)


def piece(z_refs, g, k, s):
    return z_refs[2 * g + (k & 1)][k >> 1, s]


def forward_kernel(s0, sg, has_block, ids, *refs):
    if has_block:
        block_ref, refs = refs[0], refs[1:]
    x_ref, y_ref, t_ref, w_ref, own_ref, out_ref = refs
    w = own_ref.shape[3]
    batch = x_ref.shape[0]
    dn = (((1,), (1,)), ((), ()))

    def one(s, _):
        for k in (1, 3, 0, 2):
            r = chunk(ids, k, w)
            z = lax.dot_general(t_ref[s0 + s, r], x_ref[...], dn, preferred_element_type=F32)
            z = z + lax.dot_general(w_ref[s0 + s, r], y_ref[s0 + s], dn, preferred_element_type=F32)
            if k & 1:
                row = pl.multiple_of(((k >> 1) * sg + s) * batch, batch)
                out_ref[pl.ds(row, batch)] = z.T.astype(BF16)
            else:
                own_ref[k >> 1, s] = z.T
        return 0

    lax.fori_loop(0, sg, one, 0)
    if has_block:
        out_ref[pl.ds(2 * sg * batch, EXTRA)] = block_ref[...]


def forward(ids, block, x_bf, y_bf, tech, recourse, s0, sg, n, after):
    batch, first_cols = x_bf.shape
    second_cols = y_bf.shape[2]
    w = tech.shape[1] // n
    sent = (2 * sg * batch + (0 if block is None else EXTRA), w)
    args = [ids] + ([] if block is None else [block]) + [x_bf, y_bf, tech, recourse]
    work = sg * n * w * (first_cols + second_cols)
    return call(
        functools.partial(forward_kernel, s0, sg, block is not None),
        [struct((2, sg, batch, w)), struct(sent, BF16)],
        args, BIG, smem=1, cost=(2 * batch * work * 8, 2 * work), after=after,
    )


def scalar_rows(p):
    p = p.astype(F32)
    return (p + pltpu.roll(p, EXTRA - 2, 0)) + pltpu.roll(p, EXTRA - 4, 0)


def pair_kernel(has_block, *refs):
    if has_block:
        block_ref, refs = refs[0], refs[1:]
    own_ref, other_ref, half_ref = refs
    _, sg, batch, w = own_ref.shape
    for j in range(2):
        for s in range(sg):
            rows = pl.ds((j * sg + s) * batch, batch)
            half_ref[rows] = (own_ref[j, s] + other_ref[rows].astype(F32)).astype(BF16)
    if has_block:
        rows = pl.ds(2 * sg * batch, EXTRA)
        both = scalar_rows(block_ref[:, :LANES]) + scalar_rows(other_ref[rows, :LANES])
        both = jnp.where(lax.broadcasted_iota(jnp.int32, both.shape, 0) < 2, both, 0.0)
        hi, mid, low = (p.astype(F32) for p in split3(both))
        half_ref[rows] = jnp.zeros((EXTRA, w), BF16)
        half_ref[rows, :LANES] = (hi + pltpu.roll(mid, 2, 0) + pltpu.roll(low, 4, 0)).astype(BF16)


def total_kernel(has_block, half_ref, other_ref, total_ref, *scal_refs):
    _, sg, batch, _ = total_ref.shape
    for j in range(2):
        for s in range(sg):
            mine = half_ref[pl.ds((j * sg + s) * batch, batch)].astype(F32)
            theirs = other_ref[pl.ds(((1 - j) * sg + s) * batch, batch)].astype(F32)
            total_ref[j, s] = (mine + theirs).astype(BF16)
    if has_block:
        rows = pl.ds(2 * sg * batch, EXTRA)
        both = scalar_rows(half_ref[rows, :LANES]) + scalar_rows(other_ref[rows, :LANES])
        square = jnp.concatenate([both, jnp.zeros((LANES - EXTRA, LANES), F32)], axis=0).T
        lane = lax.broadcasted_iota(jnp.int32, (batch, LANES), 1)
        scal_refs[0][...] = jnp.where(lane < 2, square[:batch], 0.0)


def adjoint_kernel(n, s0, has_q, ids, *refs):
    z_refs, refs = refs[:2], refs[2:]
    if has_q:
        q_ref, refs = refs[0], refs[1:]
    acc_ref, t_ref, w_ref, out_ref, ty_ref = refs
    _, sg, batch, w = z_refs[0].shape
    cols = t_ref.shape[2]
    if acc_ref.shape[1] > LANES:
        out_ref[:, :cols] = acc_ref[:, :cols]
    else:
        out_ref[:, :cols] = jnp.zeros((batch, cols), F32)

    def one(s, carry):
        zz, zq = carry
        ty = jnp.zeros((batch, w_ref.shape[2]), F32)
        acc = out_ref[:, :cols]
        for k in range(n):
            r = chunk(ids, k, w)
            z = piece(z_refs, 0, k, s)
            ty = ty + jnp.dot(z, w_ref[s0 + s, r], preferred_element_type=F32)
            acc = acc + jnp.dot(z, t_ref[s0 + s, r], preferred_element_type=F32)
            zf = z.astype(F32)
            zz = zz + zf * zf
            if has_q:
                zq = zq + zf * q_ref[k, s0 + s]
        ty_ref[s] = ty
        out_ref[:, :cols] = acc
        return zz, zq

    zero = jnp.zeros((batch, w), F32)
    zz, zq = lax.fori_loop(0, sg, one, (zero, zero))
    scal = acc_ref[:, acc_ref.shape[1] - LANES:]
    scal = scal + at_lane(scal.shape, 2, jnp.sum(zz, axis=1, keepdims=True))
    if has_q:
        scal = scal + at_lane(scal.shape, 3, jnp.sum(zq, axis=1, keepdims=True))
    out_ref[:, cols:] = scal


def adjoint(ids, pieces, q, acc, tech, recourse, s0, after=()):
    _, sg, batch, w = pieces[0].shape
    n = tech.shape[1] // w
    first_cols = tech.shape[2]
    second_cols = recourse.shape[2]
    args = [ids, *pieces] + ([] if q is None else [q]) + [acc, tech, recourse]
    work = sg * n * w * (first_cols + second_cols)
    return call(
        functools.partial(adjoint_kernel, n, s0, q is not None),
        [struct((batch, first_cols + LANES)), struct((sg, batch, second_cols))],
        args, BIG, smem=1, cost=(2 * batch * work * 8, 2 * work), after=after,
    )


def load_kernel(n, ids, *refs):
    d_refs, refs = refs[:-8], refs[-8:]
    t_hbm, w_hbm, tv_ref, wv_ref, out_ref, ty_ref, t_sem, w_sem = refs
    _, _, batch, w = d_refs[0].shape
    scen = t_hbm.shape[0]
    cols = t_hbm.shape[2]
    copies = []
    for s in range(scen):
        t_copy = pltpu.make_async_copy(t_hbm.at[s], tv_ref.at[s], t_sem.at[s])
        w_copy = pltpu.make_async_copy(w_hbm.at[s], wv_ref.at[s], w_sem.at[s])
        t_copy.start()
        w_copy.start()
        copies.append((t_copy, w_copy))
    acc = jnp.zeros((batch, cols), F32)
    for s in range(scen):
        t_copy, w_copy = copies[s]
        t_copy.wait()
        w_copy.wait()
        ty = jnp.zeros((batch, w_hbm.shape[2]), F32)
        for k in range(n):
            r = chunk(ids, k, w)
            g = max(j for j in range(GROUPS) if FIRST[j] <= s)
            z = piece(d_refs, g, k, s - FIRST[g])
            ty = ty + jnp.dot(z, wv_ref[s, r], preferred_element_type=F32)
            acc = acc + jnp.dot(z, tv_ref[s, r], preferred_element_type=F32)
        ty_ref[s] = ty
    out_ref[:, :cols] = acc
    out_ref[:, cols:] = jnp.zeros((batch, LANES), F32)


def load(ids, groups, tech, recourse):
    _, _, batch, w = groups[0][0].shape
    n = tech.shape[1] // w
    scen = tech.shape[0]
    pieces = [p for pieces in groups for p in pieces]
    return pl.pallas_call(
        functools.partial(load_kernel, n),
        name="load",
        in_specs=[SMEM] + [VMEM] * len(pieces) + [HBM, HBM],
        out_specs=[VMEM] * 4,
        out_shape=[
            struct(tech.shape, BF16),
            struct(recourse.shape, BF16),
            struct((batch, tech.shape[2] + LANES)),
            struct((scen, batch, recourse.shape[2])),
        ],
        scratch_shapes=[pltpu.SemaphoreType.DMA((scen,)), pltpu.SemaphoreType.DMA((scen,))],
        compiler_params=pltpu.CompilerParams(vmem_limit_bytes=BIG),
        cost_estimate=pl.CostEstimate(flops=10**10, bytes_accessed=20 << 20, transcendentals=0),
    )(ids, *pieces, tech, recourse)


def pack_kernel(a_ref, b_ref, out_ref):
    cols = a_ref.shape[1] - LANES
    out_ref[:, :cols] = (a_ref[:, :cols] + b_ref[:, :cols]).astype(BF16)
    hi, mid, low = (p.astype(F32) for p in split3(a_ref[:, cols:] + b_ref[:, cols:]))
    out_ref[:, cols:] = (hi + pltpu.roll(mid, 4, 1) + pltpu.roll(low, 8, 1)).astype(BF16)


def sum_far(part_refs):
    cols = part_refs[0].shape[1] - LANES
    vector = tree_sum([p[:, :cols].astype(F32) for p in part_refs])
    scal = []
    for p in part_refs:
        t = p[:, cols:].astype(F32)
        scal.append((t + pltpu.roll(t, LANES - 4, 1)) + pltpu.roll(t, LANES - 8, 1))
    return vector, tree_sum(scal)


def write_block(block_ref, norm, cross):
    batch = norm.shape[0]
    pieces = [p.astype(F32) for p in split3(norm)] + [p.astype(F32) for p in split3(cross)]
    square = jnp.zeros((batch, LANES), F32)
    for j, p in enumerate((pieces[0], pieces[3], pieces[1], pieces[4], pieces[2], pieces[5])):
        square = square + at_lane((batch, LANES), j, p)
    square = jnp.concatenate([square, jnp.zeros((LANES - batch, LANES), F32)], axis=0).T
    block_ref[...] = jnp.zeros_like(block_ref)
    block_ref[:, :LANES] = square[:EXTRA].astype(BF16)


def rowsum(v):
    return jnp.sum(v, axis=1, keepdims=True)


def begin_kernel(n_far, share, *refs):
    parts, refs = refs[:n_far], refs[n_far:]
    ty_ref, cx_ref, cy_ref, rx_ref, ry_ref, xb_ref, yb_ref, block_ref = refs
    vector, _ = sum_far(parts)
    res = vector - cx_ref[...]
    rx_ref[...] = res
    xb_ref[...] = res.astype(BF16)
    norm = rowsum(res * res) * share
    for s in range(ty_ref.shape[0]):
        res = ty_ref[s] - cy_ref[s]
        ry_ref[s] = res
        yb_ref[s] = res.astype(BF16)
        norm = norm + rowsum(res * res)
    write_block(block_ref, norm, norm)


def steps_of(step, scal, st):
    norm, cross, zz, zq = (scal[:, j:j + 1] for j in range(4))
    if step:
        old_norm, dd, qq = (st[:, j:j + 1] for j in range(3))
        beta = norm / old_norm
        dd = norm + 2.0 * beta * cross + beta * beta * dd
        qq = zz + 2.0 * beta * zq + beta * beta * qq
    else:
        beta = jnp.zeros_like(norm)
        dd, qq = norm, zz
    alpha = norm / (dd + qq)
    shape = scal.shape
    st = at_lane(shape, 0, norm) + at_lane(shape, 1, dd) + at_lane(shape, 2, qq)
    ab = at_lane(shape, 0, alpha) + at_lane(shape, 1, beta)
    return alpha, beta, st, ab


def update_kernel(n_far, step, share, *refs):
    parts, refs = refs[:n_far], refs[n_far:]
    if step:
        st_ref, dx_ref, dy_ref, mx_ref, my_ref = refs[:5]
        refs = refs[5:]
    ty_ref, rx_ref, ry_ref, solx_ref, soly_ref = refs[:5]
    (rxo, ryo, dxo, dyo, mxo, myo, solxo, solyo, sto, abo, xb_ref, yb_ref, block_ref) = refs[5:]
    vector, scal = sum_far(parts)
    alpha, beta, st, ab = steps_of(step, scal, st_ref[...] if step else None)
    sto[...] = st
    abo[...] = ab

    def one(res, t, d, m):
        if step:
            m = (res + t) + beta * m
            d = res + beta * d
        else:
            m = res + t
            d = res
        return res - alpha * m, d, m

    old = (dx_ref[...], mx_ref[...]) if step else (None, None)
    res, d, m = one(rx_ref[...], vector, *old)
    rxo[...] = res
    dxo[...] = d
    mxo[...] = m
    solxo[...] = solx_ref[...] + alpha * d
    xb_ref[...] = res.astype(BF16)
    norm = rowsum(res * res) * share
    cross = rowsum(res * d) * share
    for s in range(ty_ref.shape[0]):
        old = (dy_ref[s], my_ref[s]) if step else (None, None)
        res, d, m = one(ry_ref[s], ty_ref[s], *old)
        ryo[s] = res
        dyo[s] = d
        myo[s] = m
        solyo[s] = soly_ref[s] + alpha * d
        yb_ref[s] = res.astype(BF16)
        norm = norm + rowsum(res * res)
        cross = cross + rowsum(res * d)
    write_block(block_ref, norm, cross)


def row_kernel(n, groups, step, *refs):
    z_refs, refs = refs[:2 * groups], refs[2 * groups:]
    if step:
        q_ref, refs = refs[0], refs[1:]
    image_ref, ab_ref, qo, imageo = refs
    ab = ab_ref[...]
    alpha, beta = ab[:, 0:1], ab[:, 1:2]
    for g in range(groups):
        def one(j, _, g=g):
            s = FIRST[g] + j
            for k in range(n):
                q = piece(z_refs, g, k, j).astype(F32)
                if step:
                    q = q + beta * q_ref[k, s]
                qo[k, s] = q
                imageo[k, s] = image_ref[k, s] + alpha * q
            return 0

        lax.fori_loop(0, SIZES[g], one, 0)


def rowscal_kernel(n, groups, *refs):
    z_refs, refs = refs[:2 * groups], refs[2 * groups:]
    q_ref, scal_ref, out_ref = refs
    _, _, batch, w = z_refs[0].shape
    zz = jnp.zeros((batch, w), F32)
    zq = jnp.zeros((batch, w), F32)
    for g in range(groups):
        for j in range(SIZES[g]):
            for k in range(n):
                z = piece(z_refs, g, k, j).astype(F32)
                zz = zz + z * z
                zq = zq + z * q_ref[k, FIRST[g] + j]
    shape = out_ref.shape
    out_ref[...] = scal_ref[...] + at_lane(shape, 2, rowsum(zz)) + at_lane(shape, 3, rowsum(zq))


def finish_kernel(n_far, *refs):
    parts, refs = refs[:n_far], refs[n_far:]
    st_ref, dx_ref, dy_ref, rx_ref, ry_ref, solx_ref, soly_ref, solxo, solyo, abo = refs
    alpha, beta, _, ab = steps_of(1, tree_sum([p[...] for p in parts]), st_ref[...])
    abo[...] = ab
    solxo[...] = solx_ref[...] + alpha * (rx_ref[...] + beta * dx_ref[...])
    for s in range(ry_ref.shape[0]):
        solyo[s] = soly_ref[s] + alpha * (ry_ref[s] + beta * dy_ref[s])


def cone_factors(lead, tail):
    norm_tail = jnp.sqrt(tail)
    inside = norm_tail <= lead
    polar = norm_tail <= -lead
    safe = jnp.where(norm_tail > 0.0, norm_tail, 1.0)
    middle = 0.5 * (lead + norm_tail)
    head = jnp.where(inside, lead, jnp.where(polar, 0.0, middle))
    scale = jnp.where(inside, 1.0, jnp.where(polar, 0.0, middle / safe))
    return head, scale


def project_kernel(n, groups, *refs):
    z_refs, refs = refs[:2 * groups], refs[2 * groups:]
    q_ref, image_ref, ab_ref, rhs_ref, dual_ref, cone_ref, start_ref = refs[:7]
    imageo_ref, slack_ref, dualo_ref, *d_refs = refs[7:]
    _, _, b, w = rhs_ref.shape
    labels = lax.broadcasted_iota(jnp.int32, (NCONE, w), 0)
    ab = ab_ref[...]
    alpha, beta = ab[:, 0:1], ab[:, 1:2]
    for g in range(groups):
        def one(j, _, g=g):
            s = FIRST[g] + j
            values = []
            images = []
            sums = jnp.zeros((6 * b, NCONE), F32)
            for k in range(n):
                image = image_ref[k, s] + alpha * (piece(z_refs, g, k, j).astype(F32) + beta * q_ref[k, s])
                imageo_ref[k, s] = image
                v = rhs_ref[k, s] - image - dual_ref[k, s]
                st = start_ref[k, s]
                onehot = (cone_ref[k, s] == labels).astype(F32).astype(BF16)
                stack = jnp.concatenate(split3(v * st) + split3(v * v * (1.0 - st)), axis=0)
                sums = sums + lax.dot_general(
                    stack, onehot, (((1,), (1,)), ((), ())), preferred_element_type=F32
                )
                values.append(v)
                images.append(image)
            lead = (sums[2 * b:3 * b] + sums[b:2 * b]) + sums[:b]
            tail = (sums[5 * b:6 * b] + sums[4 * b:5 * b]) + sums[3 * b:4 * b]
            head, scale = cone_factors(lead, tail)
            back = jnp.concatenate(split3(head) + split3(scale), axis=0)
            for k in range(n):
                onehot = (cone_ref[k, s] == labels).astype(F32).astype(BF16)
                rows = jnp.dot(back, onehot, preferred_element_type=F32)
                head_rows = (rows[2 * b:3 * b] + rows[b:2 * b]) + rows[:b]
                scale_rows = (rows[5 * b:6 * b] + rows[4 * b:5 * b]) + rows[3 * b:4 * b]
                st = start_ref[k, s]
                slack = st * head_rows + (1.0 - st) * values[k] * scale_rows
                base = images[k] - rhs_ref[k, s]
                dual = dual_ref[k, s] + base + slack
                if k == 0:
                    slack_ref[s] = slack
                dualo_ref[k, s] = dual
                d_refs[2 * g + (k & 1)][k >> 1, j] = (-base - slack - dual).astype(BF16)
            return 0

        lax.fori_loop(0, SIZES[g], one, 0)


def body(tech, recourse, rhs, cost_first, cost_second, cone_id):
    n_scen = lax.axis_size("scen")
    n = lax.axis_size("col")
    here = lax.axis_index("col")
    scen, rows, first_cols = tech.shape
    second_cols = recourse.shape[2]
    batch = rhs.shape[0]
    w = rows // n
    share = 1.0 / n_scen
    if n != 4 or scen != sum(SIZES):
        raise ValueError("unexpected mesh")
    ids = (here ^ jnp.arange(n, dtype=jnp.int32)).astype(jnp.int32)

    def ordered(value):
        parts = [lax.dynamic_slice_in_dim(value, (here ^ k) * w, w, value.ndim - 1) for k in range(n)]
        return jnp.stack(parts)

    rhs_k = ordered(jnp.transpose(rhs, (1, 0, 2)))
    start = jnp.concatenate(
        [jnp.ones((scen, 1), F32), (cone_id[:, 1:] != cone_id[:, :-1]).astype(F32)], axis=1
    )
    start_k = ordered(start)[:, :, None, :]
    cone_k = ordered(cone_id)[:, :, None, :]
    cost_x = cost_first[None, :]
    cost_y = cost_second[:, None, :]

    far = list(range(2, n_scen, 2))
    n_far = len(far) + 1
    first_shape = struct((batch, first_cols))
    second_shape = struct((scen, batch, second_cols))
    scal_shape = struct((batch, LANES))
    block_shape = struct((EXTRA, w), BF16)
    cast_shapes = [struct(first_shape.shape, BF16), struct(second_shape.shape, BF16), block_shape]

    def far_parts(own):
        return [own] + [swap(own, "scen", n_scen, k) for k in far]

    def reduce_first(payload):
        other = swap(payload, "scen", n_scen, 1)
        (own,) = call(pack_kernel, [struct(payload.shape, BF16)], [payload, other])
        return far_parts(own)

    def apply_both(x_bf, y_bf, block, q, with_adjoint):
        token = ()
        own, sent, half, groups = {}, {}, {}, {}
        scal = None
        acc = None
        seconds = []
        for stage, g in ORDER:
          if stage == "forward":
              part = block if g == 0 else None
              own[g], sent[g] = forward(
                  ids, part, x_bf, y_bf, tech, recourse, FIRST[g], SIZES[g], n, token
              )
              token = (own[g],)
              sent[g] = swap(sent[g], "col", n, 1)
          elif stage == "pair":
              lead = [block] if g == 0 else []
              (half[g],) = call(
                  functools.partial(pair_kernel, bool(lead)),
                  [struct((2 * SIZES[g] * batch + EXTRA * len(lead), w), BF16)],
                  lead + [own[g], sent[g]], after=token,
              )
              token = (half[g],)
              sent[g] = swap(half[g], "col", n, 2)
          elif stage == "total":
              lead = [0] if g == 0 else []
              out = call(
                  functools.partial(total_kernel, bool(lead)),
                  [struct(own[g].shape, BF16)] + [scal_shape] * len(lead),
                  [half[g], sent[g]], after=token,
              )
              token = (out[0],)
              if lead:
                  scal = out[1]
              groups[g] = [out[0], swap(out[0], "col", n, 1)]
          elif with_adjoint:
              acc, second = adjoint(
                  ids, groups[g], q, scal if acc is None else acc, tech, recourse, FIRST[g], token
              )
              token = (second,)
              seconds.append(second)
        groups = [groups[g] for g in range(GROUPS)]
        if not with_adjoint:
            return groups, scal
        return groups, acc, joined(seconds)

    def joined(seconds):
        return seconds[0] if GROUPS == 1 else jnp.concatenate(seconds, axis=0)

    def apply_adjoint(groups, q, acc):
        seconds = []
        for g, pieces in enumerate(groups):
            acc, second = adjoint(ids, pieces, q, acc, tech, recourse, FIRST[g])
            seconds.append(second)
        return acc, joined(seconds)

    flat = lambda groups: [piece for pieces in groups for piece in pieces]
    sol_first = jnp.zeros(first_shape.shape, F32)
    sol_second = jnp.zeros(second_shape.shape, F32)
    dual = jnp.zeros(rhs_k.shape, F32)
    image = jnp.zeros(rhs_k.shape, F32)
    no_scal = jnp.zeros((batch, LANES), F32)
    d = rhs_k.astype(BF16)
    groups = [[d[p::2, FIRST[g]:FIRST[g] + SIZES[g]] for p in range(2)] for g in range(GROUPS)]
    for outer in range(ITERS):
        if outer == 0:
            tech, recourse, payload, ty = load(ids, groups, tech, recourse)
        else:
            payload, ty = apply_adjoint(groups, None, no_scal)
        parts = reduce_first(payload)
        rx, ry, x_bf, y_bf, block = call(
            functools.partial(begin_kernel, n_far, share),
            [first_shape, second_shape] + cast_shapes, parts + [ty, cost_x, cost_y],
        )
        q = None
        state = []
        for step in range(CG_STEPS):
            if step + 1 < CG_STEPS:
                groups, payload, ty = apply_both(x_bf, y_bf, block, q, True)
                parts = reduce_first(payload)
                (rx, ry, dx, dy, mx, my, sol_first, sol_second, st, ab, x_bf, y_bf, block) = call(
                    functools.partial(update_kernel, n_far, step, share),
                    [first_shape, second_shape] * 4 + [scal_shape] * 2 + cast_shapes,
                    parts + state + [ty, rx, ry, sol_first, sol_second],
                )
                state = [st, dx, dy, mx, my]
                q, image = call(
                    functools.partial(row_kernel, n, GROUPS, step),
                    [struct(image.shape)] * 2,
                    flat(groups) + ([] if q is None else [q]) + [image, ab],
                )
            else:
                groups, scal = apply_both(x_bf, y_bf, block, q, False)
                (scal,) = call(
                    functools.partial(rowscal_kernel, n, GROUPS), [scal_shape],
                    flat(groups) + [q, scal],
                )
                parts = far_parts(scal + swap(scal, "scen", n_scen, 1))
                sol_first, sol_second, ab = call(
                    functools.partial(finish_kernel, n_far),
                    [first_shape, second_shape, scal_shape],
                    parts + [st, dx, dy, rx, ry, sol_first, sol_second],
                )
        image, slack, dual, *ds = call(
            functools.partial(project_kernel, n, GROUPS),
            [struct(image.shape), struct(image.shape[1:]), struct(image.shape)]
            + [struct((2, SIZES[j // 2], batch, w), BF16) for j in range(2 * GROUPS)],
            flat(groups) + [q, image, ab, rhs_k, dual, cone_k, start_k], 16 << 20,
        )
        groups = [ds[2 * g:2 * g + 2] for g in range(GROUPS)]
    swap_lead = lambda value: jnp.transpose(value, (1, 0, 2))
    return sol_first, swap_lead(sol_second), swap_lead(slack), swap_lead(dual[0])


def solution(mesh):
    placed = (
        P("scen", None, "col"),
        P("scen", None, "col"),
        P(None, "scen", None),
        P("col"),
        P("scen", "col"),
        P("scen", None),
    )
    return jax.shard_map(
        body,
        mesh=mesh,
        in_specs=placed,
        out_specs=(
            P(None, "col"),
            P(None, "scen", "col"),
            P(None, "scen", "col"),
            P(None, "scen", "col"),
        ),
        check_vma=False,
    )
```

```python
import functools

import jax
import jax.numpy as jnp
from jax import lax
from jax.experimental import pallas as pl
from jax.experimental.pallas import tpu as pltpu
from jax.sharding import PartitionSpec as P


NCONE = 128
ITERS = 3
CG_STEPS = 3
SIZES = (1, 2, 1)
GROUPS = len(SIZES)
FIRST = tuple(sum(SIZES[:g]) for g in range(GROUPS))
ORDER = (
    ("forward", 0),
    ("forward", 1),
    ("pair", 0),
    ("forward", 2),
    ("pair", 1),
    ("total", 0),
    ("pair", 2),
    ("total", 1),
    ("adjoint", 0),
    ("total", 2),
    ("adjoint", 1),
    ("adjoint", 2),
)
LANES = 128
EXTRA = 8


F32 = jnp.float32
BF16 = jnp.bfloat16
VMEM = pl.BlockSpec(memory_space=pltpu.VMEM)
SMEM = pl.BlockSpec(memory_space=pltpu.SMEM)
ANY = pl.BlockSpec(memory_space=pl.ANY)
HBM = pl.BlockSpec(memory_space=pltpu.HBM)
BIG = 6 << 20
SMALL = 4 << 20


def swap(value, axis, size, k):
    return lax.ppermute(value, axis, [(j, j ^ k) for j in range(size)])


def tree_sum(parts):
    while len(parts) > 1:
        parts = [parts[j] + parts[j + 1] for j in range(0, len(parts), 2)]
    return parts[0]


def call(kernel, out_shape, args, limit=SMALL, smem=0, cost=(10**6, 10**6), after=()):
    count = len(args)

    def ordered_kernel(*refs):
        kernel(*refs[:count], *refs[count + len(after):])

    return pl.pallas_call(
        ordered_kernel if after else kernel,
        in_specs=[SMEM] * smem + [VMEM] * (count - smem) + [ANY] * len(after),
        out_specs=[VMEM] * len(out_shape),
        out_shape=out_shape,
        compiler_params=pltpu.CompilerParams(vmem_limit_bytes=limit),
        cost_estimate=pl.CostEstimate(flops=cost[0], bytes_accessed=cost[1], transcendentals=0),
    )(*args, *after)


def struct(shape, dtype=F32):
    return jax.ShapeDtypeStruct(tuple(shape), dtype)


def chunk(ids, k, w):
    return pl.ds(pl.multiple_of(ids[k] * w, w), w)


def split3(v):
    hi = v.astype(BF16)
    rest = v - hi.astype(F32)
    mid = rest.astype(BF16)
    low = (rest - mid.astype(F32)).astype(BF16)
    return hi, mid, low


def repeat(count, one, carry):
    for s in range(count):
        carry = one(s, carry)
    return carry


def at_lane(shape, j, column):
    return jnp.where(lax.broadcasted_iota(jnp.int32, shape, 1) == j, column, 0.0)


def piece(z_refs, g, k, s):
    return z_refs[2 * g + (k & 1)][k >> 1, s]


def forward_kernel(s0, sg, has_block, ids, *refs):
    if has_block:
        block_ref, refs = refs[0], refs[1:]
    x_ref, y_ref, t_ref, w_ref, own_ref, out_ref = refs
    w = own_ref.shape[3]
    batch = x_ref.shape[0]
    dn = (((1,), (1,)), ((), ()))

    def one(s, _):
        for k in (1, 3, 0, 2):
            r = chunk(ids, k, w)
            z = lax.dot_general(t_ref[s0 + s, r], x_ref[...], dn, preferred_element_type=F32)
            z = z + lax.dot_general(w_ref[s0 + s, r], y_ref[s0 + s], dn, preferred_element_type=F32)
            if k & 1:
                row = ((k >> 1) * sg + s) * batch
                out_ref[pl.ds(row, batch)] = z.T.astype(BF16)
            else:
                own_ref[k >> 1, s] = z.T
        return 0

    repeat(sg, one, 0)
    if has_block:
        out_ref[pl.ds(2 * sg * batch, EXTRA)] = block_ref[...]


def forward(ids, block, x_bf, y_bf, tech, recourse, s0, sg, n, after):
    batch, first_cols = x_bf.shape
    second_cols = y_bf.shape[2]
    w = tech.shape[1] // n
    sent = (2 * sg * batch + (0 if block is None else EXTRA), w)
    args = [ids] + ([] if block is None else [block]) + [x_bf, y_bf, tech, recourse]
    work = sg * n * w * (first_cols + second_cols)
    return call(
        functools.partial(forward_kernel, s0, sg, block is not None),
        [struct((2, sg, batch, w)), struct(sent, BF16)],
        args, BIG, smem=1, cost=(2 * batch * work * 8, 2 * work), after=after,
    )


def scalar_rows(p):
    p = p.astype(F32)
    return (p + pltpu.roll(p, EXTRA - 2, 0)) + pltpu.roll(p, EXTRA - 4, 0)


def pair_kernel(has_block, *refs):
    if has_block:
        block_ref, refs = refs[0], refs[1:]
    own_ref, other_ref, half_ref = refs
    _, sg, batch, w = own_ref.shape
    for j in range(2):
        for s in range(sg):
            rows = pl.ds((j * sg + s) * batch, batch)
            half_ref[rows] = (own_ref[j, s] + other_ref[rows].astype(F32)).astype(BF16)
    if has_block:
        rows = pl.ds(2 * sg * batch, EXTRA)
        both = scalar_rows(block_ref[:, :LANES]) + scalar_rows(other_ref[rows, :LANES])
        both = jnp.where(lax.broadcasted_iota(jnp.int32, both.shape, 0) < 2, both, 0.0)
        hi, mid, low = (p.astype(F32) for p in split3(both))
        half_ref[rows] = jnp.zeros((EXTRA, w), BF16)
        half_ref[rows, :LANES] = (hi + pltpu.roll(mid, 2, 0) + pltpu.roll(low, 4, 0)).astype(BF16)


def total_kernel(has_block, half_ref, other_ref, total_ref, *scal_refs):
    _, sg, batch, _ = total_ref.shape
    for j in range(2):
        for s in range(sg):
            mine = half_ref[pl.ds((j * sg + s) * batch, batch)].astype(F32)
            theirs = other_ref[pl.ds(((1 - j) * sg + s) * batch, batch)].astype(F32)
            total_ref[j, s] = (mine + theirs).astype(BF16)
    if has_block:
        rows = pl.ds(2 * sg * batch, EXTRA)
        both = scalar_rows(half_ref[rows, :LANES]) + scalar_rows(other_ref[rows, :LANES])
        square = jnp.concatenate([both, jnp.zeros((LANES - EXTRA, LANES), F32)], axis=0).T
        lane = lax.broadcasted_iota(jnp.int32, (batch, LANES), 1)
        scal_refs[0][...] = jnp.where(lane < 2, square[:batch], 0.0)


def adjoint_kernel(n, s0, has_q, ids, *refs):
    z_refs, refs = refs[:2], refs[2:]
    if has_q:
        q_ref, refs = refs[0], refs[1:]
    acc_ref, t_ref, w_ref, out_ref, ty_ref = refs
    _, sg, batch, w = z_refs[0].shape
    cols = t_ref.shape[2]
    if acc_ref.shape[1] > LANES:
        out_ref[:, :cols] = acc_ref[:, :cols]
    else:
        out_ref[:, :cols] = jnp.zeros((batch, cols), F32)

    def one(s, carry):
        zz, zq = carry
        ty = jnp.zeros((batch, w_ref.shape[2]), F32)
        acc = out_ref[:, :cols]
        for k in range(n):
            r = chunk(ids, k, w)
            z = piece(z_refs, 0, k, s)
            ty = ty + jnp.dot(z, w_ref[s0 + s, r], preferred_element_type=F32)
            acc = acc + jnp.dot(z, t_ref[s0 + s, r], preferred_element_type=F32)
            zf = z.astype(F32)
            zz = zz + zf * zf
            if has_q:
                zq = zq + zf * q_ref[k, s0 + s]
        ty_ref[s] = ty
        out_ref[:, :cols] = acc
        return zz, zq

    zero = jnp.zeros((batch, w), F32)
    zz, zq = repeat(sg, one, (zero, zero))
    scal = acc_ref[:, acc_ref.shape[1] - LANES:]
    scal = scal + at_lane(scal.shape, 2, jnp.sum(zz, axis=1, keepdims=True))
    if has_q:
        scal = scal + at_lane(scal.shape, 3, jnp.sum(zq, axis=1, keepdims=True))
    out_ref[:, cols:] = scal


def adjoint(ids, pieces, q, acc, tech, recourse, s0, after=()):
    _, sg, batch, w = pieces[0].shape
    n = tech.shape[1] // w
    first_cols = tech.shape[2]
    second_cols = recourse.shape[2]
    args = [ids, *pieces] + ([] if q is None else [q]) + [acc, tech, recourse]
    work = sg * n * w * (first_cols + second_cols)
    return call(
        functools.partial(adjoint_kernel, n, s0, q is not None),
        [struct((batch, first_cols + LANES)), struct((sg, batch, second_cols))],
        args, BIG, smem=1, cost=(2 * batch * work * 8, 2 * work), after=after,
    )


def load_kernel(n, ids, *refs):
    d_refs, refs = refs[:-8], refs[-8:]
    t_hbm, w_hbm, tv_ref, wv_ref, out_ref, ty_ref, t_sem, w_sem = refs
    _, _, batch, w = d_refs[0].shape
    scen = t_hbm.shape[0]
    cols = t_hbm.shape[2]
    copies = []
    for s in range(scen):
        t_copy = pltpu.make_async_copy(t_hbm.at[s], tv_ref.at[s], t_sem.at[s])
        w_copy = pltpu.make_async_copy(w_hbm.at[s], wv_ref.at[s], w_sem.at[s])
        t_copy.start()
        w_copy.start()
        copies.append((t_copy, w_copy))
    acc = jnp.zeros((batch, cols), F32)
    for s in range(scen):
        t_copy, w_copy = copies[s]
        t_copy.wait()
        w_copy.wait()
        ty = jnp.zeros((batch, w_hbm.shape[2]), F32)
        for k in range(n):
            r = chunk(ids, k, w)
            g = max(j for j in range(GROUPS) if FIRST[j] <= s)
            z = piece(d_refs, g, k, s - FIRST[g])
            ty = ty + jnp.dot(z, wv_ref[s, r], preferred_element_type=F32)
            acc = acc + jnp.dot(z, tv_ref[s, r], preferred_element_type=F32)
        ty_ref[s] = ty
    out_ref[:, :cols] = acc
    out_ref[:, cols:] = jnp.zeros((batch, LANES), F32)


def load(ids, groups, tech, recourse):
    _, _, batch, w = groups[0][0].shape
    n = tech.shape[1] // w
    scen = tech.shape[0]
    pieces = [p for pieces in groups for p in pieces]
    return pl.pallas_call(
        functools.partial(load_kernel, n),
        name="load",
        in_specs=[SMEM] + [VMEM] * len(pieces) + [HBM, HBM],
        out_specs=[VMEM] * 4,
        out_shape=[
            struct(tech.shape, BF16),
            struct(recourse.shape, BF16),
            struct((batch, tech.shape[2] + LANES)),
            struct((scen, batch, recourse.shape[2])),
        ],
        scratch_shapes=[pltpu.SemaphoreType.DMA((scen,)), pltpu.SemaphoreType.DMA((scen,))],
        compiler_params=pltpu.CompilerParams(vmem_limit_bytes=BIG),
        cost_estimate=pl.CostEstimate(flops=10**10, bytes_accessed=20 << 20, transcendentals=0),
    )(ids, *pieces, tech, recourse)


def pack_kernel(a_ref, b_ref, out_ref):
    cols = a_ref.shape[1] - LANES
    out_ref[:, :cols] = (a_ref[:, :cols] + b_ref[:, :cols]).astype(BF16)
    hi, mid, low = (p.astype(F32) for p in split3(a_ref[:, cols:] + b_ref[:, cols:]))
    out_ref[:, cols:] = (hi + pltpu.roll(mid, 4, 1) + pltpu.roll(low, 8, 1)).astype(BF16)


def sum_far(part_refs):
    cols = part_refs[0].shape[1] - LANES
    vector = tree_sum([p[:, :cols].astype(F32) for p in part_refs])
    scal = []
    for p in part_refs:
        t = p[:, cols:].astype(F32)
        scal.append((t + pltpu.roll(t, LANES - 4, 1)) + pltpu.roll(t, LANES - 8, 1))
    return vector, tree_sum(scal)


def write_block(block_ref, norm, cross):
    batch = norm.shape[0]
    pieces = [p.astype(F32) for p in split3(norm)] + [p.astype(F32) for p in split3(cross)]
    square = jnp.zeros((batch, LANES), F32)
    for j, p in enumerate((pieces[0], pieces[3], pieces[1], pieces[4], pieces[2], pieces[5])):
        square = square + at_lane((batch, LANES), j, p)
    square = jnp.concatenate([square, jnp.zeros((LANES - batch, LANES), F32)], axis=0).T
    block_ref[...] = jnp.zeros_like(block_ref)
    block_ref[:, :LANES] = square[:EXTRA].astype(BF16)


def rowsum(v):
    return jnp.sum(v, axis=1, keepdims=True)


def begin_kernel(n_far, share, *refs):
    parts, refs = refs[:n_far], refs[n_far:]
    ty_ref, cx_ref, cy_ref, rx_ref, ry_ref, xb_ref, yb_ref, block_ref = refs
    vector, _ = sum_far(parts)
    res = vector - cx_ref[...]
    rx_ref[...] = res
    xb_ref[...] = res.astype(BF16)
    norm = rowsum(res * res) * share
    for s in range(ty_ref.shape[0]):
        res = ty_ref[s] - cy_ref[s]
        ry_ref[s] = res
        yb_ref[s] = res.astype(BF16)
        norm = norm + rowsum(res * res)
    write_block(block_ref, norm, norm)


def steps_of(step, scal, st):
    norm, cross, zz, zq = (scal[:, j:j + 1] for j in range(4))
    if step:
        old_norm, dd, qq = (st[:, j:j + 1] for j in range(3))
        beta = norm / old_norm
        dd = norm + 2.0 * beta * cross + beta * beta * dd
        qq = zz + 2.0 * beta * zq + beta * beta * qq
    else:
        beta = jnp.zeros_like(norm)
        dd, qq = norm, zz
    alpha = norm / (dd + qq)
    shape = scal.shape
    st = at_lane(shape, 0, norm) + at_lane(shape, 1, dd) + at_lane(shape, 2, qq)
    ab = at_lane(shape, 0, alpha) + at_lane(shape, 1, beta)
    return alpha, beta, st, ab


def update_kernel(n_far, step, share, *refs):
    parts, refs = refs[:n_far], refs[n_far:]
    if step:
        st_ref, dx_ref, dy_ref, mx_ref, my_ref = refs[:5]
        refs = refs[5:]
    ty_ref, rx_ref, ry_ref, solx_ref, soly_ref = refs[:5]
    (rxo, ryo, dxo, dyo, mxo, myo, solxo, solyo, sto, abo, xb_ref, yb_ref, block_ref) = refs[5:]
    vector, scal = sum_far(parts)
    alpha, beta, st, ab = steps_of(step, scal, st_ref[...] if step else None)
    sto[...] = st
    abo[...] = ab

    def one(res, t, d, m):
        if step:
            m = (res + t) + beta * m
            d = res + beta * d
        else:
            m = res + t
            d = res
        return res - alpha * m, d, m

    old = (dx_ref[...], mx_ref[...]) if step else (None, None)
    res, d, m = one(rx_ref[...], vector, *old)
    rxo[...] = res
    dxo[...] = d
    mxo[...] = m
    solxo[...] = solx_ref[...] + alpha * d
    xb_ref[...] = res.astype(BF16)
    norm = rowsum(res * res) * share
    cross = rowsum(res * d) * share
    for s in range(ty_ref.shape[0]):
        old = (dy_ref[s], my_ref[s]) if step else (None, None)
        res, d, m = one(ry_ref[s], ty_ref[s], *old)
        ryo[s] = res
        dyo[s] = d
        myo[s] = m
        solyo[s] = soly_ref[s] + alpha * d
        yb_ref[s] = res.astype(BF16)
        norm = norm + rowsum(res * res)
        cross = cross + rowsum(res * d)
    write_block(block_ref, norm, cross)


def row_kernel(n, groups, step, *refs):
    z_refs, refs = refs[:2 * groups], refs[2 * groups:]
    if step:
        q_ref, refs = refs[0], refs[1:]
    image_ref, ab_ref, qo, imageo = refs
    ab = ab_ref[...]
    alpha, beta = ab[:, 0:1], ab[:, 1:2]
    for g in range(groups):
        def one(j, _, g=g):
            s = FIRST[g] + j
            for k in range(n):
                q = piece(z_refs, g, k, j).astype(F32)
                if step:
                    q = q + beta * q_ref[k, s]
                qo[k, s] = q
                imageo[k, s] = image_ref[k, s] + alpha * q
            return 0

        lax.fori_loop(0, SIZES[g], one, 0)


def rowscal_kernel(n, groups, *refs):
    z_refs, refs = refs[:2 * groups], refs[2 * groups:]
    q_ref, scal_ref, out_ref = refs
    _, _, batch, w = z_refs[0].shape
    zz = jnp.zeros((batch, w), F32)
    zq = jnp.zeros((batch, w), F32)
    for g in range(groups):
        for j in range(SIZES[g]):
            for k in range(n):
                z = piece(z_refs, g, k, j).astype(F32)
                zz = zz + z * z
                zq = zq + z * q_ref[k, FIRST[g] + j]
    shape = out_ref.shape
    out_ref[...] = scal_ref[...] + at_lane(shape, 2, rowsum(zz)) + at_lane(shape, 3, rowsum(zq))


def finish_kernel(n_far, *refs):
    parts, refs = refs[:n_far], refs[n_far:]
    st_ref, dx_ref, dy_ref, rx_ref, ry_ref, solx_ref, soly_ref, solxo, solyo, abo = refs
    alpha, beta, _, ab = steps_of(1, tree_sum([p[...] for p in parts]), st_ref[...])
    abo[...] = ab
    solxo[...] = solx_ref[...] + alpha * (rx_ref[...] + beta * dx_ref[...])
    for s in range(ry_ref.shape[0]):
        solyo[s] = soly_ref[s] + alpha * (ry_ref[s] + beta * dy_ref[s])


def cone_factors(lead, tail):
    norm_tail = jnp.sqrt(tail)
    inside = norm_tail <= lead
    polar = norm_tail <= -lead
    safe = jnp.where(norm_tail > 0.0, norm_tail, 1.0)
    middle = 0.5 * (lead + norm_tail)
    head = jnp.where(inside, lead, jnp.where(polar, 0.0, middle))
    scale = jnp.where(inside, 1.0, jnp.where(polar, 0.0, middle / safe))
    return head, scale


def project_kernel(n, groups, *refs):
    z_refs, refs = refs[:2 * groups], refs[2 * groups:]
    q_ref, image_ref, ab_ref, rhs_ref, dual_ref, cone_ref, start_ref = refs[:7]
    imageo_ref, slack_ref, dualo_ref, *d_refs = refs[7:]
    _, _, b, w = rhs_ref.shape
    labels = lax.broadcasted_iota(jnp.int32, (NCONE, w), 0)
    ab = ab_ref[...]
    alpha, beta = ab[:, 0:1], ab[:, 1:2]
    for g in range(groups):
        def one(j, _, g=g):
            s = FIRST[g] + j
            values = []
            images = []
            sums = jnp.zeros((6 * b, NCONE), F32)
            for k in range(n):
                image = image_ref[k, s] + alpha * (piece(z_refs, g, k, j).astype(F32) + beta * q_ref[k, s])
                imageo_ref[k, s] = image
                v = rhs_ref[k, s] - image - dual_ref[k, s]
                st = start_ref[k, s]
                onehot = (cone_ref[k, s] == labels).astype(F32).astype(BF16)
                stack = jnp.concatenate(split3(v * st) + split3(v * v * (1.0 - st)), axis=0)
                sums = sums + lax.dot_general(
                    stack, onehot, (((1,), (1,)), ((), ())), preferred_element_type=F32
                )
                values.append(v)
                images.append(image)
            lead = (sums[2 * b:3 * b] + sums[b:2 * b]) + sums[:b]
            tail = (sums[5 * b:6 * b] + sums[4 * b:5 * b]) + sums[3 * b:4 * b]
            head, scale = cone_factors(lead, tail)
            back = jnp.concatenate(split3(head) + split3(scale), axis=0)
            for k in range(n):
                onehot = (cone_ref[k, s] == labels).astype(F32).astype(BF16)
                rows = jnp.dot(back, onehot, preferred_element_type=F32)
                head_rows = (rows[2 * b:3 * b] + rows[b:2 * b]) + rows[:b]
                scale_rows = (rows[5 * b:6 * b] + rows[4 * b:5 * b]) + rows[3 * b:4 * b]
                st = start_ref[k, s]
                slack = st * head_rows + (1.0 - st) * values[k] * scale_rows
                base = images[k] - rhs_ref[k, s]
                dual = dual_ref[k, s] + base + slack
                if k == 0:
                    slack_ref[s] = slack
                dualo_ref[k, s] = dual
                d_refs[2 * g + (k & 1)][k >> 1, j] = (-base - slack - dual).astype(BF16)
            return 0

        lax.fori_loop(0, SIZES[g], one, 0)


def body(tech, recourse, rhs, cost_first, cost_second, cone_id):
    n_scen = lax.axis_size("scen")
    n = lax.axis_size("col")
    here = lax.axis_index("col")
    scen, rows, first_cols = tech.shape
    second_cols = recourse.shape[2]
    batch = rhs.shape[0]
    w = rows // n
    share = 1.0 / n_scen
    if n != 4 or scen != sum(SIZES):
        raise ValueError("unexpected mesh")
    ids = (here ^ jnp.arange(n, dtype=jnp.int32)).astype(jnp.int32)

    def ordered(value):
        parts = [lax.dynamic_slice_in_dim(value, (here ^ k) * w, w, value.ndim - 1) for k in range(n)]
        return jnp.stack(parts)

    rhs_k = ordered(jnp.transpose(rhs, (1, 0, 2)))
    start = jnp.concatenate(
        [jnp.ones((scen, 1), F32), (cone_id[:, 1:] != cone_id[:, :-1]).astype(F32)], axis=1
    )
    start_k = ordered(start)[:, :, None, :]
    cone_k = ordered(cone_id)[:, :, None, :]
    cost_x = cost_first[None, :]
    cost_y = cost_second[:, None, :]

    far = list(range(2, n_scen, 2))
    n_far = len(far) + 1
    first_shape = struct((batch, first_cols))
    second_shape = struct((scen, batch, second_cols))
    scal_shape = struct((batch, LANES))
    block_shape = struct((EXTRA, w), BF16)
    cast_shapes = [struct(first_shape.shape, BF16), struct(second_shape.shape, BF16), block_shape]

    def far_parts(own):
        return [own] + [swap(own, "scen", n_scen, k) for k in far]

    def reduce_first(payload):
        other = swap(payload, "scen", n_scen, 1)
        (own,) = call(pack_kernel, [struct(payload.shape, BF16)], [payload, other])
        return far_parts(own)

    def apply_both(x_bf, y_bf, block, q, with_adjoint):
        token = ()
        own, sent, half, groups = {}, {}, {}, {}
        scal = None
        acc = None
        seconds = []
        for stage, g in ORDER:
          if stage == "forward":
              part = block if g == 0 else None
              own[g], sent[g] = forward(
                  ids, part, x_bf, y_bf, tech, recourse, FIRST[g], SIZES[g], n, token
              )
              token = (own[g],)
              sent[g] = swap(sent[g], "col", n, 1)
          elif stage == "pair":
              lead = [block] if g == 0 else []
              (half[g],) = call(
                  functools.partial(pair_kernel, bool(lead)),
                  [struct((2 * SIZES[g] * batch + EXTRA * len(lead), w), BF16)],
                  lead + [own[g], sent[g]], after=token,
              )
              token = (half[g],)
              sent[g] = swap(half[g], "col", n, 2)
          elif stage == "total":
              lead = [0] if g == 0 else []
              out = call(
                  functools.partial(total_kernel, bool(lead)),
                  [struct(own[g].shape, BF16)] + [scal_shape] * len(lead),
                  [half[g], sent[g]], after=token,
              )
              token = (out[0],)
              if lead:
                  scal = out[1]
              groups[g] = [out[0], swap(out[0], "col", n, 1)]
          elif with_adjoint:
              acc, second = adjoint(
                  ids, groups[g], q, scal if acc is None else acc, tech, recourse, FIRST[g], token
              )
              token = (second,)
              seconds.append(second)
        groups = [groups[g] for g in range(GROUPS)]
        if not with_adjoint:
            return groups, scal
        return groups, acc, joined(seconds)

    def joined(seconds):
        return seconds[0] if GROUPS == 1 else jnp.concatenate(seconds, axis=0)

    def apply_adjoint(groups, q, acc):
        seconds = []
        for g, pieces in enumerate(groups):
            acc, second = adjoint(ids, pieces, q, acc, tech, recourse, FIRST[g])
            seconds.append(second)
        return acc, joined(seconds)

    flat = lambda groups: [piece for pieces in groups for piece in pieces]
    sol_first = jnp.zeros(first_shape.shape, F32)
    sol_second = jnp.zeros(second_shape.shape, F32)
    dual = jnp.zeros(rhs_k.shape, F32)
    image = jnp.zeros(rhs_k.shape, F32)
    no_scal = jnp.zeros((batch, LANES), F32)
    d = rhs_k.astype(BF16)
    groups = [[d[p::2, FIRST[g]:FIRST[g] + SIZES[g]] for p in range(2)] for g in range(GROUPS)]
    for outer in range(ITERS):
        if outer == 0:
            tech, recourse, payload, ty = load(ids, groups, tech, recourse)
        else:
            payload, ty = apply_adjoint(groups, None, no_scal)
        parts = reduce_first(payload)
        rx, ry, x_bf, y_bf, block = call(
            functools.partial(begin_kernel, n_far, share),
            [first_shape, second_shape] + cast_shapes, parts + [ty, cost_x, cost_y],
        )
        q = None
        state = []
        for step in range(CG_STEPS):
            if step + 1 < CG_STEPS:
                groups, payload, ty = apply_both(x_bf, y_bf, block, q, True)
                parts = reduce_first(payload)
                (rx, ry, dx, dy, mx, my, sol_first, sol_second, st, ab, x_bf, y_bf, block) = call(
                    functools.partial(update_kernel, n_far, step, share),
                    [first_shape, second_shape] * 4 + [scal_shape] * 2 + cast_shapes,
                    parts + state + [ty, rx, ry, sol_first, sol_second],
                )
                state = [st, dx, dy, mx, my]
                q, image = call(
                    functools.partial(row_kernel, n, GROUPS, step),
                    [struct(image.shape)] * 2,
                    flat(groups) + ([] if q is None else [q]) + [image, ab],
                )
            else:
                groups, scal = apply_both(x_bf, y_bf, block, q, False)
                (scal,) = call(
                    functools.partial(rowscal_kernel, n, GROUPS), [scal_shape],
                    flat(groups) + [q, scal],
                )
                parts = far_parts(scal + swap(scal, "scen", n_scen, 1))
                sol_first, sol_second, ab = call(
                    functools.partial(finish_kernel, n_far),
                    [first_shape, second_shape, scal_shape],
                    parts + [st, dx, dy, rx, ry, sol_first, sol_second],
                )
        image, slack, dual, *ds = call(
            functools.partial(project_kernel, n, GROUPS),
            [struct(image.shape), struct(image.shape[1:]), struct(image.shape)]
            + [struct((2, SIZES[j // 2], batch, w), BF16) for j in range(2 * GROUPS)],
            flat(groups) + [q, image, ab, rhs_k, dual, cone_k, start_k], 16 << 20,
        )
        groups = [ds[2 * g:2 * g + 2] for g in range(GROUPS)]
    swap_lead = lambda value: jnp.transpose(value, (1, 0, 2))
    return sol_first, swap_lead(sol_second), swap_lead(slack), swap_lead(dual[0])


def solution(mesh):
    placed = (
        P("scen", None, "col"),
        P("scen", None, "col"),
        P(None, "scen", None),
        P("col"),
        P("scen", "col"),
        P("scen", None),
    )
    return jax.shard_map(
        body,
        mesh=mesh,
        in_specs=placed,
        out_specs=(
            P(None, "col"),
            P(None, "scen", "col"),
            P(None, "scen", "col"),
            P(None, "scen", "col"),
        ),
        check_vma=False,
    )
```
